32 devices in a mesh: ens: 2 (over y), space: 4 (over z), chan: 2 (over x), sub: 2 (over core).
Axes of the slice: x: 2, y: 2, z: 4, core: 2. Of those that a mesh axis runs over, the one named last changes fastest.
Arguments:
- node_state: bfloat16 [8192, 512], P(('ens', 'space'), ('chan', 'sub')), parts along dimension 0, may hold values from -6 to 6
- norm_gains: float32 [2, 512], replicated, may hold values from 0.25 to 1.75
- norm_shifts: float32 [2, 512], replicated, may hold values from -3 to 3
- query_weight: bfloat16 [512, 512], P(None, 'chan')
- key_weight: bfloat16 [512, 512], P(None, 'chan')
- value_weight: bfloat16 [512, 512], P(None, 'chan'), may hold values from -0.25 to 0.25
- out_weight: bfloat16 [512, 512], replicated, may hold values from -0.25 to 0.25
- ffn_in: bfloat16 [2048, 512], P('chan'), may hold values from -0.25 to 0.25
- ffn_out: bfloat16 [2048, 512], P('chan'), may hold values from -0.125 to 0.125
- live_counts: int32 [4], P('space'), may hold values from 512 to 1024, as said below
- send_rows: int32 [4, 2, 256], P('space'), may hold values from 0 to 1023, as said below
- tile_keys: int32 [32, 12], P('space'), may hold values from 0 to 11, as said below
- tile_bits: int32 [32, 12, 4, 128], P('space'), may hold values from -2147483648 to 2147483647, as said below
Outputs:
- updated: bfloat16 [8192, 512], P(('ens', 'space'), ('chan', 'sub')), parts along dimension 0
The draws below stay inside these ranges and needn't reach their ends.
There are 2 independent parts, one for each index of `ens`. The reference program is written for one: setup_inputs(seed, part) draws one part's arguments, and reference() takes and returns one part's arrays. A program takes and returns all parts, laid end to end along the dimension named above; an argument that names none is the same for every part. Nothing has to cross between parts.
Inputs may be any that keep to these rules, and one draw needn't show every extreme that they name: Partition s has live nodes 0 to live_counts[s] - 1; the first and the last partition are full. send_rows[s, 0] lists nodes of partition s read by its lower neighbour, send_rows[s, 1] those read by its upper neighbour; all are live nodes, and entries may repeat. `tile_keys`: slot 0 of every block names the block itself (its index within the partition); other slots name blocks of the same partition (below 8), of the lower halo (from 8) or of the upper halo (from 10); the first partition names no lower halo and the last no upper halo. `tile_bits`: bit j of word w in column r of a slot says whether query r of the block may attend key 32 w + j of the slot's block (bit 31 is the sign bit); in slot 0 every query's own bit is set. Slots whose words are all zero carry no edges.
All inputs are finite; a program needn't handle non-finite values.
Results may differ from the reference program's by a relative error of at most 0.0095.
Values may be sent and summed in bfloat16 or wider, within the bound.
A program may use at most 64 MiB of HBM per device.

```python
import math
import jax
import jax.numpy as jnp
from jax import lax

D = 512
HEADS = 8
HD = 64
FF = 2048
TILE = 128
WORDS = 4
KT = 12
HBLK = 2
HB = 256
NB = 8
NBK = 12
NODE_PART = 1024
NODES = 4096
BLOCKS = 32
N_SPACE = 4


def paired_projection(key):
    shared_part = jax.random.normal(jax.random.fold_in(key, 11), (D, D), jnp.float32) / math.sqrt(D)
    second_part = jax.random.normal(jax.random.fold_in(key, 12), (D, D), jnp.float32) / math.sqrt(D)
    return (shared_part, second_part)


def draw_query_weight(key, part):
    shared_part, second_part = paired_projection(key)
    return shared_part.astype(jnp.bfloat16)


def draw_key_weight(key, part):
    shared_part, second_part = paired_projection(key)
    return second_part.astype(jnp.bfloat16)


def partition_sizes(key):
    parts_total = BLOCKS // NB
    section = jnp.arange(parts_total, dtype=jnp.int32)
    drawn = jax.random.randint(jax.random.fold_in(key, 51), (parts_total,), NODE_PART // 2, NODE_PART + 1, dtype=jnp.int32)
    polar = (section == 0) | (section == parts_total - 1)
    return jnp.where(polar, NODE_PART, drawn)


def draw_live_counts(key, part):
    return partition_sizes(key)


def draw_send_rows(key, part):
    sizes = partition_sizes(key)
    return jax.random.randint(jax.random.fold_in(key, 61), (BLOCKS // NB, 2, HB), 0, sizes[:, None, None], dtype=jnp.int32)


def slot_use(key):
    blocks = jnp.arange(BLOCKS, dtype=jnp.int32)
    section = blocks // NB
    polar = (section == 0) | (section == BLOCKS // NB - 1)
    partial_use = jax.random.randint(jax.random.fold_in(key, 21), (BLOCKS,), (KT + 1) // 2, KT + 1, dtype=jnp.int32)
    return jnp.where(polar, KT, partial_use)


def draw_tile_keys(key, part):
    blocks = jnp.arange(BLOCKS, dtype=jnp.int32)
    local_block = blocks % NB
    section = blocks // NB
    offsets = jax.random.randint(jax.random.fold_in(key, 31), (BLOCKS, KT), 1, NB, dtype=jnp.int32)
    others = (local_block[:, None] + offsets) % NB
    near_low = local_block < NB // 2
    low_pick = NB + jax.random.randint(jax.random.fold_in(key, 32), (BLOCKS,), 0, HBLK, dtype=jnp.int32)
    high_pick = NB + HBLK + jax.random.randint(jax.random.fold_in(key, 33), (BLOCKS,), 0, HBLK, dtype=jnp.int32)
    halo_pick = jnp.where(near_low, low_pick, high_pick)
    outer_side = (section == 0) & near_low | (section == BLOCKS // NB - 1) & jnp.logical_not(near_low)
    second_slot = jnp.where(outer_side, others[:, 1], halo_pick)
    return jnp.concatenate([local_block[:, None], second_slot[:, None], others[:, 2:]], axis=1)


def draw_tile_bits(key, part):
    random_words = jax.random.randint(jax.random.fold_in(key, 41), (BLOCKS, KT, WORDS, TILE), -2147483647, 2147483647, dtype=jnp.int32)
    slot_live = (jnp.arange(KT, dtype=jnp.int32)[None, :] < slot_use(key)[:, None]).astype(jnp.int32)
    random_words = random_words * slot_live[:, :, None, None]
    rows_at = jnp.arange(TILE, dtype=jnp.int32)
    own_word = jnp.arange(WORDS, dtype=jnp.int32)[:, None] == (rows_at // 32)[None, :]
    diagonal = jnp.where(own_word, jnp.left_shift(jnp.int32(1), rows_at % 32)[None, :], jnp.int32(0))
    first_slot = jnp.bitwise_or(random_words[:, :1], diagonal[None, None])
    return jnp.concatenate([first_slot, random_words[:, 1:]], axis=1)


def block_levels(key, dims, cuts, smallest, top_value):
    factor_of = 1.0
    for dim, shards_of in cuts:
        draws = jax.random.uniform(jax.random.fold_in(jax.random.fold_in(key, 6), dim), (shards_of,), jnp.float32, smallest / len(cuts), top_value / len(cuts))
        factor_of = factor_of * jnp.repeat(jnp.exp(draws), dims[dim] // shards_of).reshape((-1,) + (1,) * (len(dims) - 1 - dim))
    return factor_of


def bell_draw(rng, shape, width, bound, shards=(), kind=jnp.bfloat16):
    values = jax.random.normal(rng, shape, jnp.float32) * width
    if len(shards) > 0:
        values = block_levels(rng, shape, shards, -0.22, 0.18) * values
    return jnp.clip(values, min=-bound, max=bound).astype(kind)


def setup_inputs(seed: int = 0, part: int = 0) -> dict:
    streams_of = jax.random.split(jax.random.key(seed), 14)
    own_keys = jax.random.split(jax.random.fold_in(streams_of[13], part), 14)
    return {
        "node_state": bell_draw(own_keys[0], (NODES, D), 1.0, 6.0, ((0, 4), (1, 4))),
        "norm_gains": jnp.clip(1.0 + 0.15 * jax.random.normal(streams_of[1], (2, D), jnp.float32), 0.25, 1.75),
        "norm_shifts": bell_draw(streams_of[2], (2, D), 0.5, 3.0, (), jnp.float32),
        "query_weight": draw_query_weight(jax.random.fold_in(streams_of[13], 71), part),
        "key_weight": draw_key_weight(jax.random.fold_in(streams_of[13], 71), part),
        "value_weight": bell_draw(streams_of[5], (D, D), D ** -0.5, 0.25, ((1, 2),)),
        "out_weight": bell_draw(streams_of[6], (D, D), D ** -0.5, 0.25),
        "ffn_in": bell_draw(streams_of[7], (FF, D), D ** -0.5, 0.25, ((0, 2),)),
        "ffn_out": bell_draw(streams_of[8], (FF, D), FF ** -0.5, 0.125, ((0, 2),)),
        "live_counts": draw_live_counts(jax.random.fold_in(streams_of[13], 71), part),
        "send_rows": draw_send_rows(jax.random.fold_in(streams_of[13], 71), part),
        "tile_keys": draw_tile_keys(jax.random.fold_in(streams_of[13], 71), part),
        "tile_bits": draw_tile_bits(jax.random.fold_in(streams_of[13], 71), part),
    }


NORM_EPS = 1e-05
NEG_FILL = -1e+30

def normalize_rows(source, gain_row, shift_row):
    row_mean = lax.optimization_barrier(jnp.mean(source, axis=-1, keepdims=True))
    spread = lax.optimization_barrier(jnp.mean(source * source, axis=-1, keepdims=True)) - row_mean * row_mean
    return (source - row_mean) * lax.rsqrt(spread + NORM_EPS) * gain_row + shift_row

def unpack_allowed(key_bits, key_ids, live_count, tile_size, blocks_own):
    shifts = jnp.arange(32, dtype=jnp.int32)
    expanded = jnp.right_shift(key_bits[..., None, :], shifts[:, None]) & 1
    lead_shape = key_bits.shape[:-2]
    expanded = expanded.reshape(lead_shape + (tile_size, tile_size))
    key_index = key_ids[..., None] * tile_size + jnp.arange(tile_size, dtype=jnp.int32)
    key_live = (key_ids[..., None] >= blocks_own) | (key_index < live_count)
    slot_count = key_ids.shape[-1]
    slot_first = jnp.arange(slot_count, dtype=jnp.int32)[:, None, None] == 0
    diagonal = jnp.arange(tile_size, dtype=jnp.int32)[:, None] == jnp.arange(tile_size, dtype=jnp.int32)[None, :]
    own_bit = slot_first & diagonal[None]
    return (expanded == 1) & (key_live[..., None] | own_bit)

def reference(node_state, norm_gains, norm_shifts, query_weight, key_weight, value_weight, out_weight, ffn_in, ffn_out, live_counts, send_rows, tile_keys, tile_bits):
    float_state = node_state.astype(jnp.float32)
    normed = normalize_rows(float_state, norm_gains[0], norm_shifts[0]).astype(jnp.bfloat16)
    queries = jnp.dot(normed, query_weight, preferred_element_type=jnp.float32).astype(jnp.bfloat16)
    key_rows = jnp.dot(normed, key_weight, preferred_element_type=jnp.float32).astype(jnp.bfloat16)
    value_rows = jnp.dot(normed, value_weight, preferred_element_type=jnp.float32).astype(jnp.bfloat16)
    key_values = jnp.concatenate([key_rows, value_rows], axis=1).reshape(N_SPACE, NODE_PART, 2 * D)
    upward = jnp.take_along_axis(key_values, send_rows[:, 1, :, None], axis=1)
    downward = jnp.take_along_axis(key_values, send_rows[:, 0, :, None], axis=1)
    empty_rim = jnp.zeros((1, HB, 2 * D), key_values.dtype)
    lower_rim = jnp.concatenate([empty_rim, upward[:-1]], axis=0)
    upper_rim = jnp.concatenate([downward[1:], empty_rim], axis=0)
    extended = jnp.concatenate([key_values, lower_rim, upper_rim], axis=1).reshape(N_SPACE, NBK, TILE, 2 * D)
    query_blocks = queries.reshape(N_SPACE, NB, TILE, HEADS, HD)
    key_ids = tile_keys.reshape(N_SPACE, NB, KT)
    key_bits = tile_bits.reshape(N_SPACE, NB, KT, WORDS, TILE)
    score_scale = 1.0 / math.sqrt(HD)

    def one_partition(inputs):
        ext_part, q_part, id_part, bit_part, count_part = inputs
        chosen = ext_part[id_part]
        keys_part = chosen[..., :D].reshape(NB, KT, TILE, HEADS, HD).astype(jnp.float32)
        values_part = chosen[..., D:].reshape(NB, KT, TILE, HEADS, HD).astype(jnp.float32)
        scores = jnp.einsum('brhd,btkhd->bhrtk', q_part.astype(jnp.float32), keys_part) * score_scale
        allowed = unpack_allowed(bit_part, id_part, count_part, TILE, NB)
        allowed = jnp.transpose(allowed, (0, 3, 1, 2))[:, None]
        masked = jnp.where(allowed, scores, NEG_FILL)
        row_max = lax.optimization_barrier(jnp.max(masked, axis=(3, 4), keepdims=True))
        weights = jnp.where(allowed, jnp.exp(scores - row_max), 0.0)
        row_total = lax.optimization_barrier(jnp.sum(weights, axis=(3, 4)))
        rounded = lax.optimization_barrier(weights.astype(jnp.bfloat16)).astype(jnp.float32)
        mixed_heads = jnp.einsum('bhrtk,btkhd->brhd', rounded, values_part)
        mixed_heads = mixed_heads / jnp.transpose(row_total, (0, 2, 1))[..., None]
        return mixed_heads.astype(jnp.bfloat16).reshape(NB * TILE, D)
    attended = lax.map(one_partition, (extended, query_blocks, key_ids, key_bits, live_counts)).reshape(NODES, D)
    after_attn = float_state + jnp.dot(attended, out_weight, preferred_element_type=jnp.float32)
    normed_two = normalize_rows(after_attn, norm_gains[1], norm_shifts[1]).astype(jnp.bfloat16)
    hidden = jax.nn.gelu(jnp.dot(normed_two, ffn_in.T, preferred_element_type=jnp.float32)).astype(jnp.bfloat16)
    result = after_attn + jnp.dot(hidden, ffn_out, preferred_element_type=jnp.float32)
    node_at = jnp.arange(NODES, dtype=jnp.int32)
    node_live = node_at % NODE_PART < live_counts[node_at // NODE_PART]
    return jnp.where(node_live[:, None], result, 0.0).astype(jnp.bfloat16)
```

```python
import math

import jax
import jax.numpy as jnp
from jax import lax
from jax.experimental import pallas as pl
from jax.experimental.pallas import tpu as pltpu
from jax.sharding import PartitionSpec as P

HD = 64


NORM_EPS = 1e-05
NEG_FILL = -1e30


def padded_2(array, sides, width):
    for axis, dim in sides:
        size, length = (lax.axis_size(axis), array.shape[dim])
        up = [(i, (i + 1) % size) for i in range(size - 1)]
        down = [(j, i) for i, j in up]
        last = lax.slice_in_dim(array, length - width, length, axis=dim)
        leading = lax.slice_in_dim(array, 0, width, axis=dim)
        before = lax.ppermute(last, axis, up)
        after = lax.ppermute(leading, axis, down)
        array = jnp.concatenate([before, array, after], axis=dim)
    return array


def normalize_rows(source, gain_row, shift_row):
    row_mean = jnp.mean(source, axis=-1, keepdims=True)
    spread = jnp.mean(source * source, axis=-1, keepdims=True) - row_mean * row_mean
    return (source - row_mean) * lax.rsqrt(spread + NORM_EPS) * gain_row + shift_row


def unpack_allowed(key_bits, key_ids, live_count, tile_size, blocks_own):
    shifts = jnp.arange(32, dtype=jnp.int32)
    expanded = jnp.right_shift(key_bits[..., None, :], shifts[:, None]) & 1
    lead_shape = key_bits.shape[:-2]
    expanded = expanded.reshape(lead_shape + (tile_size, tile_size))
    key_index = key_ids[..., None] * tile_size + jnp.arange(tile_size, dtype=jnp.int32)
    key_live = (key_ids[..., None] >= blocks_own) | (key_index < live_count)
    slot_count = key_ids.shape[-1]
    slot_first = jnp.arange(slot_count, dtype=jnp.int32)[:, None, None] == 0
    diagonal = (
        jnp.arange(tile_size, dtype=jnp.int32)[:, None]
        == jnp.arange(tile_size, dtype=jnp.int32)[None, :]
    )
    own_bit = slot_first & diagonal[None]
    return (expanded == 1) & (key_live[..., None] | own_bit)


def hidden_term(rows, in_piece, out_piece):
    hidden = jax.nn.gelu(
        lax.dot_general(
            rows, in_piece, (((1,), (1,)), ((), ())), preferred_element_type=jnp.float32
        )
    ).astype(jnp.bfloat16)
    return jnp.dot(hidden, out_piece, preferred_element_type=jnp.float32)


def on_device(
    node_state,
    norm_gains,
    norm_shifts,
    query_weight,
    key_weight,
    value_weight,
    out_weight,
    ffn_in,
    ffn_out,
    live_counts,
    send_rows,
    tile_keys,
    tile_bits,
):
    n_chan = lax.axis_size("chan")
    n_sub = lax.axis_size("sub")
    groups = n_chan * n_sub
    chan_at = lax.axis_index("chan")
    sub_at = lax.axis_index("sub")
    node_rank = chan_at * n_sub + sub_at
    node_count = node_state.shape[0]
    tile_size = tile_bits.shape[-1]
    word_count = tile_bits.shape[-2]
    slot_count = tile_keys.shape[1]
    blocks_own = tile_keys.shape[0]
    per_rank = node_count // groups
    head_cols = query_weight.shape[1]
    heads_here = head_cols // HD
    halo_rows = send_rows.shape[-1]
    live_count = live_counts[0]

    def own_half(source):
        step_rows = source.shape[0] // groups
        shaped = source.reshape((n_chan, n_sub, step_rows) + source.shape[1:])
        picked = lax.dynamic_index_in_dim(shaped, sub_at, 1, keepdims=False)
        return picked.reshape((n_chan * step_rows,) + source.shape[1:])

    node_rows = lax.all_to_all(node_state, ("chan", "sub"), split_axis=0, concat_axis=1, tiled=True)
    pair_weight = jnp.concatenate([key_weight, value_weight], axis=1)
    gathered = lax.all_gather(node_state, ("chan", "sub"), axis=1, tiled=True)
    normed = normalize_rows(gathered.astype(jnp.float32), norm_gains[0], norm_shifts[0]).astype(
        jnp.bfloat16
    )
    key_values = jnp.dot(normed, pair_weight, preferred_element_type=jnp.float32).astype(
        jnp.bfloat16
    )
    queries = jnp.dot(own_half(normed), query_weight, preferred_element_type=jnp.float32).astype(
        jnp.bfloat16
    )
    send_list = send_rows.reshape(2 * halo_rows)
    outgoing = jnp.take(key_values, send_list, axis=0)
    padded = padded_2(outgoing, (("space", 0),), halo_rows)
    extended = jnp.concatenate([key_values, padded[:halo_rows], padded[-halo_rows:]], axis=0)
    key_blocks = extended.reshape(-1, tile_size, 2 * head_cols)
    key_ids = own_half(tile_keys)
    key_bits = own_half(tile_bits)
    block_total = key_ids.shape[0]
    per_round = math.gcd(block_total, 4)
    rounds = block_total // per_round
    score_scale = 1.0 / math.sqrt(HD)

    def attend(inputs):
        q_part, id_part, bit_part = inputs
        chosen = key_blocks[id_part]
        keys_part = chosen[..., :head_cols].reshape(
            per_round, slot_count, tile_size, heads_here, HD
        )
        values_part = chosen[..., head_cols:].reshape(
            per_round, slot_count, tile_size, heads_here, HD
        )
        scores = (
            jnp.einsum("grhd,gtkhd->ghrtk", q_part, keys_part, preferred_element_type=jnp.float32)
            * score_scale
        )
        allowed = unpack_allowed(bit_part, id_part, live_count, tile_size, blocks_own)
        allowed = jnp.transpose(allowed, (0, 3, 1, 2))[:, None]
        masked = jnp.where(allowed, scores, NEG_FILL)
        row_max = jnp.max(masked, axis=(3, 4), keepdims=True)
        weights = jnp.where(allowed, jnp.exp(scores - row_max), 0.0)
        row_total = jnp.sum(weights, axis=(3, 4))
        mixed_heads = jnp.einsum(
            "ghrtk,gtkhd->grhd",
            weights.astype(jnp.bfloat16),
            values_part,
            preferred_element_type=jnp.float32,
        )
        mixed_heads = mixed_heads / jnp.transpose(row_total, (0, 2, 1))[..., None]
        return mixed_heads.astype(jnp.bfloat16).reshape(per_round * tile_size, head_cols)

    query_groups = queries.reshape(rounds, per_round, tile_size, heads_here, HD)
    attended = lax.map(
        attend,
        (
            query_groups,
            key_ids.reshape(rounds, per_round, slot_count),
            key_bits.reshape(rounds, per_round, slot_count, word_count, tile_size),
        ),
    )
    mixed_rows = jnp.dot(
        lax.all_to_all(
            attended.reshape(n_chan, per_rank, head_cols),
            "chan",
            split_axis=0,
            concat_axis=2,
            tiled=True,
        )[0],
        out_weight,
        preferred_element_type=jnp.float32,
    )
    after_attn = node_rows.astype(jnp.float32) + mixed_rows
    normed_two = normalize_rows(after_attn, norm_gains[1], norm_shifts[1]).astype(jnp.bfloat16)
    all_rows = lax.all_gather(normed_two, "chan", axis=0, tiled=True)
    update = lax.psum_scatter(
        hidden_term(all_rows, ffn_in, ffn_out).astype(jnp.bfloat16),
        "chan",
        scatter_dimension=0,
        tiled=True,
    ).astype(jnp.float32)
    position = node_rank * per_rank + jnp.arange(per_rank, dtype=jnp.int32)
    result = jnp.where((position < live_count)[:, None], after_attn + update, 0.0).astype(
        jnp.bfloat16
    )
    return lax.all_to_all(result, ("chan", "sub"), split_axis=1, concat_axis=0, tiled=True)


MESH = pl.DeviceIdType.MESH
LOG2E = 1.4426950408889634
NT = (((1,), (1,)), ((), ()))


def gelu_tanh(u):
    inner = 0.7978845608028654 * (u + 0.044715 * (u * u * u))
    return 0.5 * u * (1.0 + jnp.tanh(inner))


def layer_kernel(
    x_ref,
    gains_ref,
    shifts_ref,
    wq_hbm,
    wk_hbm,
    wv_hbm,
    wo_hbm,
    fin_hbm,
    fout_hbm,
    live_ref,
    send_ref,
    tk_ref,
    bits_ref,
    out_ref,
    gx,
    hsend,
    nbuf,
    kbuf,
    vbuf,
    wvt,
    qbuf,
    bias_ref,
    att,
    own_part,
    psend,
    precv,
    osend,
    wq,
    wk,
    wv,
    wo,
    fin,
    fout,
    w_sem,
    loc_sem,
    a_send,
    a_recv,
    b_send,
    b_recv,
    c_send,
    c_recv,
    z_send,
    z_recv,
    t_send,
    t_recv,
    p_send,
    p_recv,
    o_send,
    o_recv,
):
    f32, bf16 = jnp.float32, jnp.bfloat16
    rows, cols = x_ref.shape
    groups, ext_rows, _ = gx.shape
    tile = bits_ref.shape[-1]
    words = bits_ref.shape[-2]
    slots = tk_ref.shape[1]
    blocks_own = tk_ref.shape[0]
    halo = send_ref.shape[-1]
    head_cols = wq.shape[1]
    pairs = head_cols // (2 * HD)
    pw = 2 * HD
    half_rows = rows // 2
    blocks_here = blocks_own // 2
    chunk = 2 * tile
    n_own = rows // chunk
    n_halo = 2 * halo // chunk
    per = chunk // tile

    c = lax.axis_index("chan")
    s = lax.axis_index("sub")
    z = lax.axis_index("space")
    nz = lax.axis_size("space")
    own = c * 2 + s
    xslot = (1 - c) * 2 + s
    xdev = {"chan": 1 - c}
    sdev = {"sub": 1 - s}
    has_up = z < nz - 1
    has_down = z > 0

    weights = ((wk_hbm, wk), (wv_hbm, wv), (wq_hbm, wq), (wo_hbm, wo), (fin_hbm, fin), (fout_hbm, fout))
    w_copies = [pltpu.make_async_copy(a, b, w_sem.at[i]) for i, (a, b) in enumerate(weights)]
    for w_copy in w_copies:
        w_copy.start()
    local = pltpu.make_async_copy(x_ref, gx.at[own, pl.ds(0, rows)], loc_sem)
    local.start()

    barrier = pltpu.get_barrier_semaphore()
    pl.semaphore_signal(barrier, inc=1, device_id=xdev, device_id_type=MESH)
    pl.semaphore_signal(barrier, inc=1, device_id=sdev, device_id_type=MESH)

    @pl.when(has_up)
    def _():
        pl.semaphore_signal(barrier, inc=1, device_id={"space": z + 1}, device_id_type=MESH)

    @pl.when(has_down)
    def _():
        pl.semaphore_signal(barrier, inc=1, device_id={"space": z - 1}, device_id_type=MESH)

    pl.semaphore_wait(barrier, 2 + jnp.where(has_up, 1, 0) + jnp.where(has_down, 1, 0))

    def rdma(src, dst, ss, rs, dev):
        return pltpu.make_async_remote_copy(
            src_ref=src, dst_ref=dst, send_sem=ss, recv_sem=rs, device_id=dev, device_id_type=MESH
        )

    def a_copy():
        return rdma(x_ref, gx.at[own, pl.ds(0, rows)], a_send.at[0], a_recv.at[0], sdev)

    def b_copy(i):
        at = pl.ds(i * chunk, chunk)
        return rdma(x_ref.at[at], gx.at[own, at], b_send.at[i], b_recv.at[i], xdev)

    def c_copy(i):
        at = pl.ds(i * chunk, chunk)
        return rdma(gx.at[xslot, at], gx.at[xslot, at], c_send.at[i], c_recv.at[i], sdev)

    tail_at = pl.ds(rows, 2 * halo)

    def a2_copy():
        return rdma(gx.at[own, tail_at], gx.at[own, tail_at], a_send.at[1], a_recv.at[1], sdev)

    def b2_copy():
        return rdma(gx.at[own, tail_at], gx.at[own, tail_at], b_send.at[n_own], b_recv.at[n_own], xdev)

    def c2_copy():
        return rdma(
            gx.at[xslot, tail_at], gx.at[xslot, tail_at], c_send.at[n_own], c_recv.at[n_own], sdev
        )

    def up_copy():
        return rdma(
            hsend.at[1], gx.at[own, pl.ds(rows, halo)], z_send.at[1], z_recv.at[1], {"space": z + 1}
        )

    def down_copy():
        return rdma(
            hsend.at[0],
            gx.at[own, pl.ds(rows + halo, halo)],
            z_send.at[0],
            z_recv.at[0],
            {"space": z - 1},
        )

    for i in range(n_own):
        b_copy(i).start()
    a_copy().start()

    lanes = lax.broadcasted_iota(jnp.int32, (halo, tile), 1)
    for side in range(2):
        wanted = jnp.broadcast_to(send_ref[0, side : side + 1, :], (tile, halo)).T
        picks = jnp.concatenate(
            [(wanted == lanes + k * tile).astype(f32).astype(bf16) for k in range(rows // tile)],
            axis=1,
        )
        hsend[side] = jnp.dot(picks, x_ref[...], preferred_element_type=f32).astype(bf16)

    @pl.when(has_up)
    def _():
        up_copy().start()

    @pl.when(has_down)
    def _():
        down_copy().start()

    @pl.when(jnp.logical_not(has_down))
    def _():
        gx[own, pl.ds(rows, halo)] = jnp.zeros((halo, cols), bf16)

    @pl.when(jnp.logical_not(has_up))
    def _():
        gx[own, pl.ds(rows + halo, halo)] = jnp.zeros((halo, cols), bf16)

    w_copies[0].wait()
    w_copies[1].wait()
    wvt[...] = wv[...].astype(f32).T.astype(bf16)
    local.wait()
    a_copy().wait_recv()

    def full_rows(at):
        return jnp.concatenate([gx[g, at] for g in range(groups)], axis=1).astype(f32)

    def norm(v, which):
        mean = jnp.mean(v, axis=-1, keepdims=True)
        spread = jnp.mean(v * v, axis=-1, keepdims=True) - mean * mean
        scaled = (v - mean) * lax.rsqrt(spread + NORM_EPS)
        return scaled * gains_ref[which : which + 1, :] + shifts_ref[which : which + 1, :]

    def project(i, keep):
        at = pl.ds(pl.multiple_of(i * chunk, chunk), chunk)
        normed = norm(full_rows(at), 0).astype(bf16)
        if keep:
            nbuf[at] = normed
        keys = jnp.dot(normed, wk[...], preferred_element_type=f32).astype(bf16)
        values = lax.dot_general(wvt[...], normed, NT, preferred_element_type=f32).astype(bf16)
        for k in range(per):
            kbuf[i * per + k] = keys[k * tile : (k + 1) * tile]
            vbuf[i * per + k] = values[:, k * tile : (k + 1) * tile]

    b_copy(0).wait_recv()
    c_copy(0).start()

    def own_step(i, carry):
        b_copy(i).wait_recv()
        c_copy(i).start()
        c_copy(i - 1).wait_recv()
        project(i - 1, True)
        return carry

    lax.fori_loop(1, n_own - 1, own_step, 0)

    @pl.when(has_down)
    def _():
        up_copy().wait_recv()

    @pl.when(has_up)
    def _():
        down_copy().wait_recv()

    b2_copy().start()
    a2_copy().start()
    lax.fori_loop(n_own - 1, n_own, own_step, 0)
    c_copy(n_own - 1).wait_recv()
    project(n_own - 1, True)

    w_copies[2].wait()
    own_at = pl.ds(pl.multiple_of(s * half_rows, half_rows), half_rows)
    qbuf[...] = jnp.dot(nbuf[own_at], wq[...], preferred_element_type=f32).astype(bf16)
    b2_copy().wait_recv()
    c2_copy().start()
    a2_copy().wait_recv()
    c2_copy().wait_recv()

    def halo_step(i, carry):
        project(i, False)
        return carry

    lax.fori_loop(n_own, n_own + n_halo, halo_step, 0)

    live = live_ref[0]
    word_rows = tile // words
    row_id = lax.broadcasted_iota(jnp.int32, (tile, tile), 0)
    col_id = lax.broadcasted_iota(jnp.int32, (tile, tile), 1)
    shifts = lax.broadcasted_iota(jnp.int32, (word_rows, tile), 0)
    low_half = lax.broadcasted_iota(jnp.int32, (tile, pw), 1) < HD
    scale = LOG2E / math.sqrt(HD)

    def t_copy(j):
        at = pl.ds(j * tile, tile)
        return rdma(att.at[c, at], att.at[c, at], t_send.at[j], t_recv.at[j], xdev)

    def attend_block(j, carry):
        b = s * blocks_here + j
        ids = [tk_ref[b, t] for t in range(slots)]
        for t in range(slots):
            block_bits = bits_ref[b, t]
            set_bits = jnp.concatenate(
                [
                    jnp.right_shift(
                        jnp.broadcast_to(block_bits[w : w + 1, :], (word_rows, tile)), shifts
                    )
                    & 1
                    for w in range(words)
                ],
                axis=0,
            )
            limit = jnp.where(ids[t] >= blocks_own, tile, live - ids[t] * tile)
            good = row_id < limit
            if t == 0:
                good = good | (row_id == col_id)
            bias_ref[t * tile : (t + 1) * tile] = jnp.where(
                (set_bits == 1) & good, 0.0, NEG_FILL
            )
        pieces = []
        q_rows = qbuf[pl.ds(pl.multiple_of(j * tile, tile), tile)]
        for pair in range(pairs):
            at = slice(pair * pw, (pair + 1) * pw)
            q_pair = q_rows[:, at]
            zero = jnp.zeros_like(q_pair)
            q_wide = jnp.concatenate(
                [jnp.where(low_half, q_pair, zero), jnp.where(low_half, zero, q_pair)], axis=0
            )
            k_all = jnp.concatenate([kbuf[ids[t]][:, at] for t in range(slots)], axis=0)
            scores = lax.dot_general(k_all, q_wide, NT, preferred_element_type=f32) * scale
            bias = bias_ref[...]
            scores = scores + jnp.concatenate([bias, bias], axis=1)
            top = jnp.max(scores, axis=0, keepdims=True)
            p = jnp.exp2(scores - top)
            total = jnp.sum(p, axis=0, keepdims=True)
            v_all = jnp.concatenate([vbuf[ids[t]][at, :] for t in range(slots)], axis=1)
            mixed = jnp.dot(v_all, p.astype(bf16), preferred_element_type=f32) / total
            pieces.append(mixed[:HD, :tile])
            pieces.append(mixed[HD:, tile:])
        att[c, pl.ds(pl.multiple_of(j * tile, tile), tile)] = (
            jnp.concatenate(pieces, axis=0).T.astype(bf16)
        )
        t_copy(j).start()
        return carry

    lax.fori_loop(0, blocks_here, attend_block, 0)

    for i in (3, 4, 5):
        w_copies[i].wait()

    n_ffn = half_rows // chunk

    def p_copy(i):
        at = pl.ds(i * chunk, chunk)
        return rdma(psend.at[at], precv.at[at], p_send.at[i], p_recv.at[i], xdev)

    def ffn_chunk(i, carry):
        for k in range(per):
            t_copy(i * per + k).wait_recv()
        at = pl.ds(pl.multiple_of(i * chunk, chunk), chunk)
        rows_at = pl.ds(pl.multiple_of(s * half_rows + i * chunk, chunk), chunk)
        mixed = jnp.concatenate([att[g, at] for g in range(groups // 2)], axis=1)
        after = full_rows(rows_at) + jnp.dot(mixed, wo[...], preferred_element_type=f32)
        normed_two = norm(after, 1).astype(bf16)
        hidden = gelu_tanh(
            lax.dot_general(normed_two, fin[...], NT, preferred_element_type=f32)
        ).astype(bf16)
        part = jnp.dot(hidden, fout[...], preferred_element_type=f32)
        left, right = part[:, :head_cols], part[:, head_cols:]
        first = c == 0
        psend[at] = jnp.where(first, right, left).astype(bf16)
        p_copy(i).start()
        own_part[at] = jnp.where(first, left + after[:, :head_cols], right + after[:, head_cols:])
        return carry

    lax.fori_loop(0, n_ffn, ffn_chunk, 0)

    def o_copy(i):
        at = pl.ds(i * chunk, chunk)
        out_at = pl.ds(s * half_rows + i * chunk, chunk)
        return rdma(osend.at[at], out_ref.at[out_at], o_send.at[i], o_recv.at[i], sdev)

    def finish(i, carry):
        p_copy(i).wait_recv()
        at = pl.ds(pl.multiple_of(i * chunk, chunk), chunk)
        base = s * half_rows + i * chunk
        summed = own_part[at] + precv[at].astype(f32)
        position = base + lax.broadcasted_iota(jnp.int32, (chunk, head_cols), 0)
        done = jnp.where(position < live, summed, 0.0)
        left, right = done[:, :cols], done[:, cols:]
        first = s == 0
        osend[at] = jnp.where(first, right, left).astype(bf16)
        o_copy(i).start()
        out_ref[pl.ds(pl.multiple_of(base, chunk), chunk)] = jnp.where(
            first, left, right
        ).astype(bf16)
        return carry

    lax.fori_loop(0, n_ffn, finish, 0)

    a_copy().wait_send()
    a2_copy().wait_send()
    b2_copy().wait_send()
    c2_copy().wait_send()
    for i in range(n_own):
        b_copy(i).wait_send()
        c_copy(i).wait_send()
    for j in range(blocks_here):
        t_copy(j).wait_send()

    @pl.when(has_up)
    def _():
        up_copy().wait_send()

    @pl.when(has_down)
    def _():
        down_copy().wait_send()

    for i in range(n_ffn):
        p_copy(i).wait_send()
        o_copy(i).wait()


def one_kernel(*args):
    (x, gains, shifts, wq, wk, wv, wo, fin, fout, live, send, tk, bits) = args
    bf16 = jnp.bfloat16
    rows, cols = x.shape
    width = gains.shape[1]
    groups = lax.axis_size("chan") * lax.axis_size("sub")
    halo = send.shape[-1]
    tile = bits.shape[-1]
    slots = tk.shape[1]
    ext = rows + 2 * halo
    head_cols = wq.shape[1]
    half = rows // 2
    chunk = 2 * tile
    n_own = rows // chunk
    blocks_here = tk.shape[0] // 2
    n_ffn = half // chunk
    vmem = pltpu.VMEM
    dma = pltpu.SemaphoreType.DMA
    in_vmem = pl.BlockSpec(memory_space=pltpu.VMEM)
    in_smem = pl.BlockSpec(memory_space=pltpu.SMEM)
    in_any = pl.BlockSpec(memory_space=pl.ANY)
    return pl.pallas_call(
        layer_kernel,
        out_shape=jax.ShapeDtypeStruct(x.shape, bf16),
        in_specs=[in_vmem] * 3 + [in_any] * 6 + [in_smem, in_vmem, in_smem, in_vmem],
        out_specs=in_vmem,
        scratch_shapes=[
            vmem((groups, ext, cols), bf16),
            vmem((2, halo, cols), bf16),
            vmem((rows, width), bf16),
            vmem((ext // tile, tile, head_cols), bf16),
            vmem((ext // tile, head_cols, tile), bf16),
            vmem((head_cols, width), bf16),
            vmem((half, head_cols), bf16),
            vmem((slots * tile, tile), jnp.float32),
            vmem((2, half, head_cols), bf16),
            vmem((half, head_cols), jnp.float32),
            vmem((half, head_cols), bf16),
            vmem((half, head_cols), bf16),
            vmem((half, cols), bf16),
            vmem(wq.shape, bf16),
            vmem(wk.shape, bf16),
            vmem(wv.shape, bf16),
            vmem(wo.shape, bf16),
            vmem(fin.shape, bf16),
            vmem(fout.shape, bf16),
            dma((6,)),
            dma,
            dma((2,)),
            dma((2,)),
            dma((n_own + 1,)),
            dma((n_own + 1,)),
            dma((n_own + 1,)),
            dma((n_own + 1,)),
            dma((2,)),
            dma((2,)),
            dma((blocks_here,)),
            dma((blocks_here,)),
            dma((n_ffn,)),
            dma((n_ffn,)),
            dma((n_ffn,)),
            dma((n_ffn,)),
        ],
        compiler_params=pltpu.CompilerParams(collective_id=0, has_side_effects=True),
    )(*args)


def on_any_device(*args):
    two_by_two = lax.axis_size("chan") == 2 and lax.axis_size("sub") == 2
    cols, head_cols = args[0].shape[1], args[3].shape[1]
    tile, halo = args[12].shape[-1], args[10].shape[-1]
    rows_fit = args[0].shape[0] % (4 * tile) == 0 and 2 * halo % (2 * tile) == 0
    if two_by_two and cols % 128 == 0 and head_cols % (2 * HD) == 0 and rows_fit:
        return one_kernel(*args)
    return on_device(*args)


def solution(mesh):
    in_specs = (
        P(("ens", "space"), ("chan", "sub")),
        P(),
        P(),
        P(None, "chan"),
        P(None, "chan"),
        P(None, "chan"),
        P(),
        P("chan", None),
        P("chan", None),
        P("space"),
        P("space", None, None),
        P("space", None),
        P("space", None, None, None),
    )
    out_specs = P(("ens", "space"), ("chan", "sub"))
    return jax.shard_map(
        on_any_device, mesh=mesh, in_specs=in_specs, out_specs=out_specs, check_vma=False
    )
```

```python
import math

import jax
import jax.numpy as jnp
from jax import lax
from jax.experimental import pallas as pl
from jax.experimental.pallas import tpu as pltpu
from jax.sharding import PartitionSpec as P

HD = 64


NORM_EPS = 1e-05
NEG_FILL = -1e30


def padded_2(array, sides, width):
    for axis, dim in sides:
        size, length = (lax.axis_size(axis), array.shape[dim])
        up = [(i, (i + 1) % size) for i in range(size - 1)]
        down = [(j, i) for i, j in up]
        last = lax.slice_in_dim(array, length - width, length, axis=dim)
        leading = lax.slice_in_dim(array, 0, width, axis=dim)
        before = lax.ppermute(last, axis, up)
        after = lax.ppermute(leading, axis, down)
        array = jnp.concatenate([before, array, after], axis=dim)
    return array


def normalize_rows(source, gain_row, shift_row):
    row_mean = jnp.mean(source, axis=-1, keepdims=True)
    spread = jnp.mean(source * source, axis=-1, keepdims=True) - row_mean * row_mean
    return (source - row_mean) * lax.rsqrt(spread + NORM_EPS) * gain_row + shift_row


def unpack_allowed(key_bits, key_ids, live_count, tile_size, blocks_own):
    shifts = jnp.arange(32, dtype=jnp.int32)
    expanded = jnp.right_shift(key_bits[..., None, :], shifts[:, None]) & 1
    lead_shape = key_bits.shape[:-2]
    expanded = expanded.reshape(lead_shape + (tile_size, tile_size))
    key_index = key_ids[..., None] * tile_size + jnp.arange(tile_size, dtype=jnp.int32)
    key_live = (key_ids[..., None] >= blocks_own) | (key_index < live_count)
    slot_count = key_ids.shape[-1]
    slot_first = jnp.arange(slot_count, dtype=jnp.int32)[:, None, None] == 0
    diagonal = (
        jnp.arange(tile_size, dtype=jnp.int32)[:, None]
        == jnp.arange(tile_size, dtype=jnp.int32)[None, :]
    )
    own_bit = slot_first & diagonal[None]
    return (expanded == 1) & (key_live[..., None] | own_bit)


def hidden_term(rows, in_piece, out_piece):
    hidden = jax.nn.gelu(
        lax.dot_general(
            rows, in_piece, (((1,), (1,)), ((), ())), preferred_element_type=jnp.float32
        )
    ).astype(jnp.bfloat16)
    return jnp.dot(hidden, out_piece, preferred_element_type=jnp.float32)


def on_device(
    node_state,
    norm_gains,
    norm_shifts,
    query_weight,
    key_weight,
    value_weight,
    out_weight,
    ffn_in,
    ffn_out,
    live_counts,
    send_rows,
    tile_keys,
    tile_bits,
):
    n_chan = lax.axis_size("chan")
    n_sub = lax.axis_size("sub")
    groups = n_chan * n_sub
    chan_at = lax.axis_index("chan")
    sub_at = lax.axis_index("sub")
    node_rank = chan_at * n_sub + sub_at
    node_count = node_state.shape[0]
    tile_size = tile_bits.shape[-1]
    word_count = tile_bits.shape[-2]
    slot_count = tile_keys.shape[1]
    blocks_own = tile_keys.shape[0]
    per_rank = node_count // groups
    head_cols = query_weight.shape[1]
    heads_here = head_cols // HD
    halo_rows = send_rows.shape[-1]
    live_count = live_counts[0]

    def own_half(source):
        step_rows = source.shape[0] // groups
        shaped = source.reshape((n_chan, n_sub, step_rows) + source.shape[1:])
        picked = lax.dynamic_index_in_dim(shaped, sub_at, 1, keepdims=False)
        return picked.reshape((n_chan * step_rows,) + source.shape[1:])

    node_rows = lax.all_to_all(node_state, ("chan", "sub"), split_axis=0, concat_axis=1, tiled=True)
    pair_weight = jnp.concatenate([key_weight, value_weight], axis=1)
    gathered = lax.all_gather(node_state, ("chan", "sub"), axis=1, tiled=True)
    normed = normalize_rows(gathered.astype(jnp.float32), norm_gains[0], norm_shifts[0]).astype(
        jnp.bfloat16
    )
    key_values = jnp.dot(normed, pair_weight, preferred_element_type=jnp.float32).astype(
        jnp.bfloat16
    )
    queries = jnp.dot(own_half(normed), query_weight, preferred_element_type=jnp.float32).astype(
        jnp.bfloat16
    )
    send_list = send_rows.reshape(2 * halo_rows)
    outgoing = jnp.take(key_values, send_list, axis=0)
    padded = padded_2(outgoing, (("space", 0),), halo_rows)
    extended = jnp.concatenate([key_values, padded[:halo_rows], padded[-halo_rows:]], axis=0)
    key_blocks = extended.reshape(-1, tile_size, 2 * head_cols)
    key_ids = own_half(tile_keys)
    key_bits = own_half(tile_bits)
    block_total = key_ids.shape[0]
    per_round = math.gcd(block_total, 4)
    rounds = block_total // per_round
    score_scale = 1.0 / math.sqrt(HD)

    def attend(inputs):
        q_part, id_part, bit_part = inputs
        chosen = key_blocks[id_part]
        keys_part = chosen[..., :head_cols].reshape(
            per_round, slot_count, tile_size, heads_here, HD
        )
        values_part = chosen[..., head_cols:].reshape(
            per_round, slot_count, tile_size, heads_here, HD
        )
        scores = (
            jnp.einsum("grhd,gtkhd->ghrtk", q_part, keys_part, preferred_element_type=jnp.float32)
            * score_scale
        )
        allowed = unpack_allowed(bit_part, id_part, live_count, tile_size, blocks_own)
        allowed = jnp.transpose(allowed, (0, 3, 1, 2))[:, None]
        masked = jnp.where(allowed, scores, NEG_FILL)
        row_max = jnp.max(masked, axis=(3, 4), keepdims=True)
        weights = jnp.where(allowed, jnp.exp(scores - row_max), 0.0)
        row_total = jnp.sum(weights, axis=(3, 4))
        mixed_heads = jnp.einsum(
            "ghrtk,gtkhd->grhd",
            weights.astype(jnp.bfloat16),
            values_part,
            preferred_element_type=jnp.float32,
        )
        mixed_heads = mixed_heads / jnp.transpose(row_total, (0, 2, 1))[..., None]
        return mixed_heads.astype(jnp.bfloat16).reshape(per_round * tile_size, head_cols)

    query_groups = queries.reshape(rounds, per_round, tile_size, heads_here, HD)
    attended = lax.map(
        attend,
        (
            query_groups,
            key_ids.reshape(rounds, per_round, slot_count),
            key_bits.reshape(rounds, per_round, slot_count, word_count, tile_size),
        ),
    )
    mixed_rows = jnp.dot(
        lax.all_to_all(
            attended.reshape(n_chan, per_rank, head_cols),
            "chan",
            split_axis=0,
            concat_axis=2,
            tiled=True,
        )[0],
        out_weight,
        preferred_element_type=jnp.float32,
    )
    after_attn = node_rows.astype(jnp.float32) + mixed_rows
    normed_two = normalize_rows(after_attn, norm_gains[1], norm_shifts[1]).astype(jnp.bfloat16)
    all_rows = lax.all_gather(normed_two, "chan", axis=0, tiled=True)
    update = lax.psum_scatter(
        hidden_term(all_rows, ffn_in, ffn_out).astype(jnp.bfloat16),
        "chan",
        scatter_dimension=0,
        tiled=True,
    ).astype(jnp.float32)
    position = node_rank * per_rank + jnp.arange(per_rank, dtype=jnp.int32)
    result = jnp.where((position < live_count)[:, None], after_attn + update, 0.0).astype(
        jnp.bfloat16
    )
    return lax.all_to_all(result, ("chan", "sub"), split_axis=1, concat_axis=0, tiled=True)


MESH = pl.DeviceIdType.MESH
LOG2E = 1.4426950408889634
NT = (((1,), (1,)), ((), ()))


def gelu_tanh(u):
    inner = 0.7978845608028654 * (u + 0.044715 * (u * u * u))
    return 0.5 * u * (1.0 + jnp.tanh(inner))


def layer_kernel(
    x_hbm,
    gains_hbm,
    shifts_hbm,
    wq_hbm,
    wk_hbm,
    wv_hbm,
    wo_hbm,
    fin_hbm,
    fout_hbm,
    live_ref,
    send_hbm,
    tk_ref,
    bits_hbm,
    out_ref,
    gx,
    hsend,
    nbuf,
    kbuf,
    vbuf,
    wvt,
    qbuf,
    s_ref,
    att,
    own_part,
    psend,
    precv,
    osend,
    wq,
    wk,
    wv,
    wo,
    fin,
    fout,
    gains_ref,
    shifts_ref,
    send_ref,
    bits_ref,
    w_sem,
    loc_sem,
    a_send,
    a_recv,
    b_send,
    b_recv,
    c_send,
    c_recv,
    z_send,
    z_recv,
    t_send,
    t_recv,
    p_send,
    p_recv,
    o_send,
    o_recv,
):
    f32, bf16 = jnp.float32, jnp.bfloat16
    rows, cols = x_hbm.shape
    groups, ext_rows, _ = gx.shape
    tile = bits_hbm.shape[-1]
    words = bits_hbm.shape[-2]
    slots = tk_ref.shape[1]
    blocks_own = tk_ref.shape[0]
    halo = send_hbm.shape[-1]
    head_cols = wq.shape[1]
    pairs = head_cols // (2 * HD)
    pw = 2 * HD
    half_rows = rows // 2
    blocks_here = blocks_own // 2
    chunk = 2 * tile
    n_own = rows // chunk
    n_halo = 2 * halo // chunk
    per = chunk // tile

    c = lax.axis_index("chan")
    s = lax.axis_index("sub")
    z = lax.axis_index("space")
    nz = lax.axis_size("space")
    own = c * 2 + s
    xslot = (1 - c) * 2 + s
    xdev = {"chan": 1 - c}
    sdev = {"sub": 1 - s}
    has_up = z < nz - 1
    has_down = z > 0

    local = pltpu.make_async_copy(x_hbm, gx.at[own, pl.ds(0, rows)], loc_sem)
    local.start()
    loads = (
        (send_hbm, send_ref),
        (wv_hbm, wv),
        (gains_hbm, gains_ref),
        (shifts_hbm, shifts_ref),
        (wk_hbm, wk),
        (wq_hbm, wq),
        (bits_hbm, bits_ref),
        (wo_hbm, wo),
        (fin_hbm, fin),
        (fout_hbm, fout),
    )
    w_copies = [pltpu.make_async_copy(a, b, w_sem.at[i]) for i, (a, b) in enumerate(loads)]

    barrier = pltpu.get_barrier_semaphore()
    pl.semaphore_signal(barrier, inc=1, device_id=xdev, device_id_type=MESH)
    pl.semaphore_signal(barrier, inc=1, device_id=sdev, device_id_type=MESH)

    @pl.when(has_up)
    def _():
        pl.semaphore_signal(barrier, inc=1, device_id={"space": z + 1}, device_id_type=MESH)

    @pl.when(has_down)
    def _():
        pl.semaphore_signal(barrier, inc=1, device_id={"space": z - 1}, device_id_type=MESH)

    for w_copy in w_copies:
        w_copy.start()
    pl.semaphore_wait(barrier, 2 + jnp.where(has_up, 1, 0) + jnp.where(has_down, 1, 0))

    def rdma(src, dst, ss, rs, dev):
        return pltpu.make_async_remote_copy(
            src_ref=src, dst_ref=dst, send_sem=ss, recv_sem=rs, device_id=dev, device_id_type=MESH
        )

    def a_copy():
        return rdma(gx.at[own, pl.ds(0, rows)], gx.at[own, pl.ds(0, rows)], a_send.at[0], a_recv.at[0], sdev)

    def b_copy(i):
        at = pl.ds(i * chunk, chunk)
        return rdma(gx.at[own, at], gx.at[own, at], b_send.at[i], b_recv.at[i], xdev)

    def c_copy(i):
        at = pl.ds(i * chunk, chunk)
        return rdma(gx.at[xslot, at], gx.at[xslot, at], c_send.at[i], c_recv.at[i], sdev)

    tail_at = pl.ds(rows, 2 * halo)

    def a2_copy():
        return rdma(gx.at[own, tail_at], gx.at[own, tail_at], a_send.at[1], a_recv.at[1], sdev)

    def b2_copy():
        return rdma(gx.at[own, tail_at], gx.at[own, tail_at], b_send.at[n_own], b_recv.at[n_own], xdev)

    def c2_copy():
        return rdma(
            gx.at[xslot, tail_at], gx.at[xslot, tail_at], c_send.at[n_own], c_recv.at[n_own], sdev
        )

    def up_copy():
        return rdma(
            hsend.at[1], gx.at[own, pl.ds(rows, halo)], z_send.at[1], z_recv.at[1], {"space": z + 1}
        )

    def down_copy():
        return rdma(
            hsend.at[0],
            gx.at[own, pl.ds(rows + halo, halo)],
            z_send.at[0],
            z_recv.at[0],
            {"space": z - 1},
        )

    local.wait()
    for i in range(n_own):
        b_copy(i).start()
    a_copy().start()
    w_copies[0].wait()

    lanes = lax.broadcasted_iota(jnp.int32, (halo, tile), 1)
    for side in range(2):
        wanted = jnp.broadcast_to(send_ref[0, side : side + 1, :], (tile, halo)).T
        picks = jnp.concatenate(
            [(wanted == lanes + k * tile).astype(f32).astype(bf16) for k in range(rows // tile)],
            axis=1,
        )
        hsend[side] = jnp.dot(picks, gx[own, pl.ds(0, rows)], preferred_element_type=f32).astype(bf16)

    @pl.when(has_up)
    def _():
        up_copy().start()

    @pl.when(has_down)
    def _():
        down_copy().start()

    @pl.when(jnp.logical_not(has_down))
    def _():
        gx[own, pl.ds(rows, halo)] = jnp.zeros((halo, cols), bf16)

    @pl.when(jnp.logical_not(has_up))
    def _():
        gx[own, pl.ds(rows + halo, halo)] = jnp.zeros((halo, cols), bf16)

    for i in range(1, 5):
        w_copies[i].wait()
    wvt[...] = wv[...].astype(f32).T.astype(bf16)
    a_copy().wait_recv()

    def full_rows(at):
        return jnp.concatenate([gx[g, at] for g in range(groups)], axis=1).astype(f32)

    def norm(v, which):
        mean = jnp.mean(v, axis=-1, keepdims=True)
        spread = jnp.mean(v * v, axis=-1, keepdims=True) - mean * mean
        scaled = (v - mean) * lax.rsqrt(spread + NORM_EPS)
        return scaled * gains_ref[which : which + 1, :] + shifts_ref[which : which + 1, :]

    def project(i, keep):
        at = pl.ds(pl.multiple_of(i * chunk, chunk), chunk)
        normed = norm(full_rows(at), 0).astype(bf16)
        if keep:
            nbuf[at] = normed
        keys = jnp.dot(normed, wk[...], preferred_element_type=f32).astype(bf16)
        values = lax.dot_general(wvt[...], normed, NT, preferred_element_type=f32).astype(bf16)
        for k in range(per):
            kbuf[i * per + k] = keys[k * tile : (k + 1) * tile]
            vbuf[i * per + k] = values[:, k * tile : (k + 1) * tile]

    b_copy(0).wait_recv()
    c_copy(0).start()

    def own_step(i, carry):
        b_copy(i).wait_recv()
        c_copy(i).start()
        c_copy(i - 1).wait_recv()
        project(i - 1, True)
        return carry

    lax.fori_loop(1, n_own - 1, own_step, 0)

    @pl.when(has_down)
    def _():
        up_copy().wait_recv()

    @pl.when(has_up)
    def _():
        down_copy().wait_recv()

    b2_copy().start()
    a2_copy().start()
    lax.fori_loop(n_own - 1, n_own, own_step, 0)
    c_copy(n_own - 1).wait_recv()
    project(n_own - 1, True)

    scale = LOG2E / math.sqrt(HD)
    w_copies[5].wait()
    own_at = pl.ds(pl.multiple_of(s * half_rows, half_rows), half_rows)
    q_rows = jnp.dot(nbuf[own_at], wq[...], preferred_element_type=f32) * scale
    qbuf[...] = q_rows.astype(bf16)
    w_copies[6].wait()
    b2_copy().wait_recv()
    c2_copy().start()
    a2_copy().wait_recv()
    c2_copy().wait_recv()

    def halo_step(i, carry):
        project(i, False)
        return carry

    lax.fori_loop(n_own, n_own + n_halo, halo_step, 0)

    live = live_ref[0]
    word_rows = tile // words
    row_id = lax.broadcasted_iota(jnp.int32, (tile, tile), 0)
    col_id = lax.broadcasted_iota(jnp.int32, (tile, tile), 1)
    shifts = lax.broadcasted_iota(jnp.int32, (word_rows, tile), 0)
    low_half = lax.broadcasted_iota(jnp.int32, (tile, pw), 1) < HD

    def t_copy(j):
        at = pl.ds(j * tile, tile)
        return rdma(att.at[c, at], att.at[c, at], t_send.at[j], t_recv.at[j], xdev)

    ones = jnp.ones((16, 2 * tile), bf16)

    def attend_block(j, carry):
        b = s * blocks_here + j
        ids = [tk_ref[b, t] for t in range(slots)]
        q_rows = qbuf[pl.ds(pl.multiple_of(j * tile, tile), tile)]
        wide = []
        for pair in range(pairs):
            q_pair = q_rows[:, pair * pw : (pair + 1) * pw]
            zero = jnp.zeros_like(q_pair)
            wide.append(
                jnp.concatenate(
                    [jnp.where(low_half, q_pair, zero), jnp.where(low_half, zero, q_pair)], axis=0
                )
            )
        tops = [jnp.full((8, 2 * tile), NEG_FILL, f32) for _ in range(pairs)]
        for t in range(slots):
            block_bits = bits_ref[b, t]
            set_bits = jnp.concatenate(
                [
                    jnp.right_shift(
                        jnp.broadcast_to(block_bits[w : w + 1, :], (word_rows, tile)), shifts
                    )
                    & 1
                    for w in range(words)
                ],
                axis=0,
            )
            limit = jnp.where(ids[t] >= blocks_own, tile, live - ids[t] * tile)
            good = row_id < limit
            if t == 0:
                good = good | (row_id == col_id)
            bias = jnp.where((set_bits == 1) & good, 0.0, NEG_FILL)
            bias = jnp.concatenate([bias, bias], axis=1)
            for pair in range(pairs):
                keys = kbuf[ids[t], :, pair * pw : (pair + 1) * pw]
                scores = lax.dot_general(keys, wide[pair], NT, preferred_element_type=f32) + bias
                s_ref[pair, t * tile : (t + 1) * tile] = scores
                tops[pair] = jnp.maximum(
                    tops[pair], jnp.max(scores.reshape(tile // 8, 8, 2 * tile), axis=0)
                )
        pieces = []
        for pair in range(pairs):
            top = jnp.max(tops[pair], axis=0, keepdims=True)
            mixed = jnp.zeros((pw + 16, 2 * tile), f32)
            for t in range(0, slots, 2):
                p = jnp.exp2(s_ref[pair, t * tile : (t + 2) * tile] - top).astype(bf16)
                at = slice(pair * pw, (pair + 1) * pw)
                values = jnp.concatenate([vbuf[ids[t], at], vbuf[ids[t + 1], at]], axis=1)
                values = jnp.concatenate([values, ones], axis=0)
                mixed = mixed + jnp.dot(values, p, preferred_element_type=f32)
            inverse = 1.0 / mixed[pw : pw + 1]
            pieces.append(mixed[:HD, :tile] * inverse[:, :tile])
            pieces.append(mixed[HD:pw, tile:] * inverse[:, tile:])
        att[c, pl.ds(pl.multiple_of(j * tile, tile), tile)] = (
            jnp.concatenate(pieces, axis=0).T.astype(bf16)
        )
        t_copy(j).start()
        return carry

    lax.fori_loop(0, blocks_here, attend_block, 0)

    for i in (7, 8, 9):
        w_copies[i].wait()

    n_ffn = half_rows // chunk

    def p_copy(i):
        at = pl.ds(i * chunk, chunk)
        return rdma(psend.at[at], precv.at[at], p_send.at[i], p_recv.at[i], xdev)

    def ffn_chunk(i, carry):
        for k in range(per):
            t_copy(i * per + k).wait_recv()
        at = pl.ds(pl.multiple_of(i * chunk, chunk), chunk)
        rows_at = pl.ds(pl.multiple_of(s * half_rows + i * chunk, chunk), chunk)
        mixed = jnp.concatenate([att[g, at] for g in range(groups // 2)], axis=1)
        after = full_rows(rows_at) + jnp.dot(mixed, wo[...], preferred_element_type=f32)
        normed_two = norm(after, 1).astype(bf16)
        hidden = gelu_tanh(
            lax.dot_general(normed_two, fin[...], NT, preferred_element_type=f32)
        ).astype(bf16)
        part = jnp.dot(hidden, fout[...], preferred_element_type=f32)
        left, right = part[:, :head_cols], part[:, head_cols:]
        first = c == 0
        psend[at] = jnp.where(first, right, left).astype(bf16)
        p_copy(i).start()
        own_part[at] = jnp.where(first, left + after[:, :head_cols], right + after[:, head_cols:])
        return carry

    lax.fori_loop(0, n_ffn, ffn_chunk, 0)

    def o_copy(i):
        at = pl.ds(i * chunk, chunk)
        out_at = pl.ds(s * half_rows + i * chunk, chunk)
        return rdma(osend.at[at], out_ref.at[out_at], o_send.at[i], o_recv.at[i], sdev)

    def finish(i, carry):
        p_copy(i).wait_recv()
        at = pl.ds(pl.multiple_of(i * chunk, chunk), chunk)
        base = s * half_rows + i * chunk
        summed = own_part[at] + precv[at].astype(f32)
        position = base + lax.broadcasted_iota(jnp.int32, (chunk, head_cols), 0)
        done = jnp.where(position < live, summed, 0.0)
        left, right = done[:, :cols], done[:, cols:]
        first = s == 0
        osend[at] = jnp.where(first, right, left).astype(bf16)
        o_copy(i).start()
        out_ref[pl.ds(pl.multiple_of(base, chunk), chunk)] = jnp.where(
            first, left, right
        ).astype(bf16)
        return carry

    lax.fori_loop(0, n_ffn, finish, 0)

    a_copy().wait_send()
    a2_copy().wait_send()
    b2_copy().wait_send()
    c2_copy().wait_send()
    for i in range(n_own):
        b_copy(i).wait_send()
        c_copy(i).wait_send()
    for j in range(blocks_here):
        t_copy(j).wait_send()

    @pl.when(has_up)
    def _():
        up_copy().wait_send()

    @pl.when(has_down)
    def _():
        down_copy().wait_send()

    for i in range(n_ffn):
        p_copy(i).wait_send()
        o_copy(i).wait()


def one_kernel(*args):
    (x, gains, shifts, wq, wk, wv, wo, fin, fout, live, send, tk, bits) = args
    bf16 = jnp.bfloat16
    rows, cols = x.shape
    width = gains.shape[1]
    groups = lax.axis_size("chan") * lax.axis_size("sub")
    halo = send.shape[-1]
    tile = bits.shape[-1]
    slots = tk.shape[1]
    ext = rows + 2 * halo
    head_cols = wq.shape[1]
    half = rows // 2
    chunk = 2 * tile
    n_own = rows // chunk
    blocks_here = tk.shape[0] // 2
    n_ffn = half // chunk
    vmem = pltpu.VMEM
    dma = pltpu.SemaphoreType.DMA
    in_vmem = pl.BlockSpec(memory_space=pltpu.VMEM)
    in_smem = pl.BlockSpec(memory_space=pltpu.SMEM)
    in_any = pl.BlockSpec(memory_space=pl.ANY)
    return pl.pallas_call(
        layer_kernel,
        out_shape=jax.ShapeDtypeStruct(x.shape, bf16),
        in_specs=[in_any] * 9 + [in_smem, in_any, in_smem, in_any],
        out_specs=in_vmem,
        scratch_shapes=[
            vmem((groups, ext, cols), bf16),
            vmem((2, halo, cols), bf16),
            vmem((rows, width), bf16),
            vmem((ext // tile, tile, head_cols), bf16),
            vmem((ext // tile, head_cols, tile), bf16),
            vmem((head_cols, width), bf16),
            vmem((half, head_cols), bf16),
            vmem((head_cols // (2 * HD), slots * tile, 2 * tile), jnp.float32),
            vmem((2, half, head_cols), bf16),
            vmem((half, head_cols), jnp.float32),
            vmem((half, head_cols), bf16),
            vmem((half, head_cols), bf16),
            vmem((half, cols), bf16),
            vmem(wq.shape, bf16),
            vmem(wk.shape, bf16),
            vmem(wv.shape, bf16),
            vmem(wo.shape, bf16),
            vmem(fin.shape, bf16),
            vmem(fout.shape, bf16),
            vmem(gains.shape, jnp.float32),
            vmem(shifts.shape, jnp.float32),
            vmem(send.shape, jnp.int32),
            vmem(bits.shape, jnp.int32),
            dma((10,)),
            dma,
            dma((2,)),
            dma((2,)),
            dma((n_own + 1,)),
            dma((n_own + 1,)),
            dma((n_own + 1,)),
            dma((n_own + 1,)),
            dma((2,)),
            dma((2,)),
            dma((blocks_here,)),
            dma((blocks_here,)),
            dma((n_ffn,)),
            dma((n_ffn,)),
            dma((n_ffn,)),
            dma((n_ffn,)),
        ],
        compiler_params=pltpu.CompilerParams(collective_id=0, has_side_effects=True),
    )(*args)


def on_any_device(*args):
    two_by_two = lax.axis_size("chan") == 2 and lax.axis_size("sub") == 2
    cols, head_cols = args[0].shape[1], args[3].shape[1]
    tile, halo = args[12].shape[-1], args[10].shape[-1]
    rows_fit = args[0].shape[0] % (4 * tile) == 0 and 2 * halo % (2 * tile) == 0
    if two_by_two and cols % 128 == 0 and head_cols % (2 * HD) == 0 and rows_fit and args[11].shape[1] % 2 == 0:
        return one_kernel(*args)
    return on_device(*args)


def solution(mesh):
    in_specs = (
        P(("ens", "space"), ("chan", "sub")),
        P(),
        P(),
        P(None, "chan"),
        P(None, "chan"),
        P(None, "chan"),
        P(),
        P("chan", None),
        P("chan", None),
        P("space"),
        P("space", None, None),
        P("space", None),
        P("space", None, None, None),
    )
    out_specs = P(("ens", "space"), ("chan", "sub"))
    return jax.shard_map(
        on_any_device, mesh=mesh, in_specs=in_specs, out_specs=out_specs, check_vma=False
    )
```

```python
import math

import jax
import jax.numpy as jnp
from jax import lax
from jax.experimental import pallas as pl
from jax.experimental.pallas import tpu as pltpu
from jax.sharding import PartitionSpec as P

HD = 64


NORM_EPS = 1e-05
NEG_FILL = -1e30


def padded_2(array, sides, width):
    for axis, dim in sides:
        size, length = (lax.axis_size(axis), array.shape[dim])
        up = [(i, (i + 1) % size) for i in range(size - 1)]
        down = [(j, i) for i, j in up]
        last = lax.slice_in_dim(array, length - width, length, axis=dim)
        leading = lax.slice_in_dim(array, 0, width, axis=dim)
        before = lax.ppermute(last, axis, up)
        after = lax.ppermute(leading, axis, down)
        array = jnp.concatenate([before, array, after], axis=dim)
    return array


def normalize_rows(source, gain_row, shift_row):
    row_mean = jnp.mean(source, axis=-1, keepdims=True)
    spread = jnp.mean(source * source, axis=-1, keepdims=True) - row_mean * row_mean
    return (source - row_mean) * lax.rsqrt(spread + NORM_EPS) * gain_row + shift_row


def unpack_allowed(key_bits, key_ids, live_count, tile_size, blocks_own):
    shifts = jnp.arange(32, dtype=jnp.int32)
    expanded = jnp.right_shift(key_bits[..., None, :], shifts[:, None]) & 1
    lead_shape = key_bits.shape[:-2]
    expanded = expanded.reshape(lead_shape + (tile_size, tile_size))
    key_index = key_ids[..., None] * tile_size + jnp.arange(tile_size, dtype=jnp.int32)
    key_live = (key_ids[..., None] >= blocks_own) | (key_index < live_count)
    slot_count = key_ids.shape[-1]
    slot_first = jnp.arange(slot_count, dtype=jnp.int32)[:, None, None] == 0
    diagonal = (
        jnp.arange(tile_size, dtype=jnp.int32)[:, None]
        == jnp.arange(tile_size, dtype=jnp.int32)[None, :]
    )
    own_bit = slot_first & diagonal[None]
    return (expanded == 1) & (key_live[..., None] | own_bit)


def hidden_term(rows, in_piece, out_piece):
    hidden = jax.nn.gelu(
        lax.dot_general(
            rows, in_piece, (((1,), (1,)), ((), ())), preferred_element_type=jnp.float32
        )
    ).astype(jnp.bfloat16)
    return jnp.dot(hidden, out_piece, preferred_element_type=jnp.float32)


def on_device(
    node_state,
    norm_gains,
    norm_shifts,
    query_weight,
    key_weight,
    value_weight,
    out_weight,
    ffn_in,
    ffn_out,
    live_counts,
    send_rows,
    tile_keys,
    tile_bits,
):
    n_chan = lax.axis_size("chan")
    n_sub = lax.axis_size("sub")
    groups = n_chan * n_sub
    chan_at = lax.axis_index("chan")
    sub_at = lax.axis_index("sub")
    node_rank = chan_at * n_sub + sub_at
    node_count = node_state.shape[0]
    tile_size = tile_bits.shape[-1]
    word_count = tile_bits.shape[-2]
    slot_count = tile_keys.shape[1]
    blocks_own = tile_keys.shape[0]
    per_rank = node_count // groups
    head_cols = query_weight.shape[1]
    heads_here = head_cols // HD
    halo_rows = send_rows.shape[-1]
    live_count = live_counts[0]

    def own_half(source):
        step_rows = source.shape[0] // groups
        shaped = source.reshape((n_chan, n_sub, step_rows) + source.shape[1:])
        picked = lax.dynamic_index_in_dim(shaped, sub_at, 1, keepdims=False)
        return picked.reshape((n_chan * step_rows,) + source.shape[1:])

    node_rows = lax.all_to_all(node_state, ("chan", "sub"), split_axis=0, concat_axis=1, tiled=True)
    pair_weight = jnp.concatenate([key_weight, value_weight], axis=1)
    gathered = lax.all_gather(node_state, ("chan", "sub"), axis=1, tiled=True)
    normed = normalize_rows(gathered.astype(jnp.float32), norm_gains[0], norm_shifts[0]).astype(
        jnp.bfloat16
    )
    key_values = jnp.dot(normed, pair_weight, preferred_element_type=jnp.float32).astype(
        jnp.bfloat16
    )
    queries = jnp.dot(own_half(normed), query_weight, preferred_element_type=jnp.float32).astype(
        jnp.bfloat16
    )
    send_list = send_rows.reshape(2 * halo_rows)
    outgoing = jnp.take(key_values, send_list, axis=0)
    padded = padded_2(outgoing, (("space", 0),), halo_rows)
    extended = jnp.concatenate([key_values, padded[:halo_rows], padded[-halo_rows:]], axis=0)
    key_blocks = extended.reshape(-1, tile_size, 2 * head_cols)
    key_ids = own_half(tile_keys)
    key_bits = own_half(tile_bits)
    block_total = key_ids.shape[0]
    per_round = math.gcd(block_total, 4)
    rounds = block_total // per_round
    score_scale = 1.0 / math.sqrt(HD)

    def attend(inputs):
        q_part, id_part, bit_part = inputs
        chosen = key_blocks[id_part]
        keys_part = chosen[..., :head_cols].reshape(
            per_round, slot_count, tile_size, heads_here, HD
        )
        values_part = chosen[..., head_cols:].reshape(
            per_round, slot_count, tile_size, heads_here, HD
        )
        scores = (
            jnp.einsum("grhd,gtkhd->ghrtk", q_part, keys_part, preferred_element_type=jnp.float32)
            * score_scale
        )
        allowed = unpack_allowed(bit_part, id_part, live_count, tile_size, blocks_own)
        allowed = jnp.transpose(allowed, (0, 3, 1, 2))[:, None]
        masked = jnp.where(allowed, scores, NEG_FILL)
        row_max = jnp.max(masked, axis=(3, 4), keepdims=True)
        weights = jnp.where(allowed, jnp.exp(scores - row_max), 0.0)
        row_total = jnp.sum(weights, axis=(3, 4))
        mixed_heads = jnp.einsum(
            "ghrtk,gtkhd->grhd",
            weights.astype(jnp.bfloat16),
            values_part,
            preferred_element_type=jnp.float32,
        )
        mixed_heads = mixed_heads / jnp.transpose(row_total, (0, 2, 1))[..., None]
        return mixed_heads.astype(jnp.bfloat16).reshape(per_round * tile_size, head_cols)

    query_groups = queries.reshape(rounds, per_round, tile_size, heads_here, HD)
    attended = lax.map(
        attend,
        (
            query_groups,
            key_ids.reshape(rounds, per_round, slot_count),
            key_bits.reshape(rounds, per_round, slot_count, word_count, tile_size),
        ),
    )
    mixed_rows = jnp.dot(
        lax.all_to_all(
            attended.reshape(n_chan, per_rank, head_cols),
            "chan",
            split_axis=0,
            concat_axis=2,
            tiled=True,
        )[0],
        out_weight,
        preferred_element_type=jnp.float32,
    )
    after_attn = node_rows.astype(jnp.float32) + mixed_rows
    normed_two = normalize_rows(after_attn, norm_gains[1], norm_shifts[1]).astype(jnp.bfloat16)
    all_rows = lax.all_gather(normed_two, "chan", axis=0, tiled=True)
    update = lax.psum_scatter(
        hidden_term(all_rows, ffn_in, ffn_out).astype(jnp.bfloat16),
        "chan",
        scatter_dimension=0,
        tiled=True,
    ).astype(jnp.float32)
    position = node_rank * per_rank + jnp.arange(per_rank, dtype=jnp.int32)
    result = jnp.where((position < live_count)[:, None], after_attn + update, 0.0).astype(
        jnp.bfloat16
    )
    return lax.all_to_all(result, ("chan", "sub"), split_axis=1, concat_axis=0, tiled=True)


MESH = pl.DeviceIdType.MESH
LOG2E = 1.4426950408889634
NT = (((1,), (1,)), ((), ()))


def gelu_tanh(u):
    inner = 0.7978845608028654 * (u + 0.044715 * (u * u * u))
    return 0.5 * u * (1.0 + jnp.tanh(inner))


def layer_kernel(
    x_hbm,
    gains_hbm,
    shifts_hbm,
    wq_hbm,
    wk_hbm,
    wv_hbm,
    wo_hbm,
    fin_hbm,
    fout_hbm,
    live_ref,
    send_hbm,
    tk_ref,
    bits_hbm,
    out_ref,
    gx,
    hsend,
    nbuf,
    kbuf,
    vbuf,
    wvt,
    qbuf,
    s_ref,
    att,
    own_part,
    psend,
    precv,
    osend,
    wq,
    wk,
    wv,
    wo,
    fin,
    fout,
    gains_ref,
    shifts_ref,
    send_ref,
    bits_ref,
    w_sem,
    loc_sem,
    a_send,
    a_recv,
    b_send,
    b_recv,
    c_send,
    c_recv,
    z_send,
    z_recv,
    t_send,
    t_recv,
    p_send,
    p_recv,
    o_send,
    o_recv,
):
    f32, bf16 = jnp.float32, jnp.bfloat16
    rows, cols = x_hbm.shape
    groups, ext_rows, _ = gx.shape
    tile = bits_hbm.shape[-1]
    words = bits_hbm.shape[-2]
    slots = tk_ref.shape[1]
    blocks_own = tk_ref.shape[0]
    halo = send_hbm.shape[-1]
    head_cols = wq.shape[1]
    pairs = head_cols // (2 * HD)
    pw = 2 * HD
    half_rows = rows // 2
    blocks_here = blocks_own // 2
    chunk = 2 * tile
    n_own = rows // chunk
    n_halo = 2 * halo // chunk
    per = chunk // tile

    c = lax.axis_index("chan")
    s = lax.axis_index("sub")
    z = lax.axis_index("space")
    nz = lax.axis_size("space")
    own = c * 2 + s
    xslot = (1 - c) * 2 + s
    xdev = {"chan": 1 - c}
    sdev = {"sub": 1 - s}
    has_up = z < nz - 1
    has_down = z > 0

    local = pltpu.make_async_copy(x_hbm, gx.at[own, pl.ds(0, rows)], loc_sem)
    local.start()
    loads = (
        (send_hbm, send_ref),
        (wv_hbm, wv),
        (gains_hbm, gains_ref),
        (shifts_hbm, shifts_ref),
        (wk_hbm, wk),
        (wq_hbm, wq),
        (bits_hbm, bits_ref),
        (wo_hbm, wo),
        (fin_hbm, fin),
        (fout_hbm, fout),
    )
    w_copies = [pltpu.make_async_copy(a, b, w_sem.at[i]) for i, (a, b) in enumerate(loads)]

    barrier = pltpu.get_barrier_semaphore()
    pl.semaphore_signal(barrier, inc=1, device_id=xdev, device_id_type=MESH)
    pl.semaphore_signal(barrier, inc=1, device_id=sdev, device_id_type=MESH)

    @pl.when(has_up)
    def _():
        pl.semaphore_signal(barrier, inc=1, device_id={"space": z + 1}, device_id_type=MESH)

    @pl.when(has_down)
    def _():
        pl.semaphore_signal(barrier, inc=1, device_id={"space": z - 1}, device_id_type=MESH)

    for w_copy in w_copies:
        w_copy.start()
    pl.semaphore_wait(barrier, 2 + jnp.where(has_up, 1, 0) + jnp.where(has_down, 1, 0))

    def rdma(src, dst, ss, rs, dev):
        return pltpu.make_async_remote_copy(
            src_ref=src, dst_ref=dst, send_sem=ss, recv_sem=rs, device_id=dev, device_id_type=MESH
        )

    def a_copy():
        return rdma(gx.at[own, pl.ds(0, rows)], gx.at[own, pl.ds(0, rows)], a_send.at[0], a_recv.at[0], sdev)

    def b_copy(i):
        at = pl.ds(i * chunk, chunk)
        return rdma(gx.at[own, at], gx.at[own, at], b_send.at[i], b_recv.at[i], xdev)

    def c_copy(i):
        at = pl.ds(i * chunk, chunk)
        return rdma(gx.at[xslot, at], gx.at[xslot, at], c_send.at[i], c_recv.at[i], sdev)

    tail_at = pl.ds(rows, 2 * halo)

    def a2_copy():
        return rdma(gx.at[own, tail_at], gx.at[own, tail_at], a_send.at[1], a_recv.at[1], sdev)

    def b2_copy():
        return rdma(gx.at[own, tail_at], gx.at[own, tail_at], b_send.at[n_own], b_recv.at[n_own], xdev)

    def c2_copy():
        return rdma(
            gx.at[xslot, tail_at], gx.at[xslot, tail_at], c_send.at[n_own], c_recv.at[n_own], sdev
        )

    def up_copy():
        return rdma(
            hsend.at[1], gx.at[own, pl.ds(rows, halo)], z_send.at[1], z_recv.at[1], {"space": z + 1}
        )

    def down_copy():
        return rdma(
            hsend.at[0],
            gx.at[own, pl.ds(rows + halo, halo)],
            z_send.at[0],
            z_recv.at[0],
            {"space": z - 1},
        )

    local.wait()
    for i in range(n_own):
        b_copy(i).start()
    a_copy().start()
    w_copies[0].wait()

    lanes = lax.broadcasted_iota(jnp.int32, (halo, tile), 1)
    for side in range(2):
        wanted = jnp.broadcast_to(send_ref[0, side : side + 1, :], (tile, halo)).T
        picks = jnp.concatenate(
            [(wanted == lanes + k * tile).astype(f32).astype(bf16) for k in range(rows // tile)],
            axis=1,
        )
        hsend[side] = jnp.dot(picks, gx[own, pl.ds(0, rows)], preferred_element_type=f32).astype(bf16)

    @pl.when(has_up)
    def _():
        up_copy().start()

    @pl.when(has_down)
    def _():
        down_copy().start()

    @pl.when(jnp.logical_not(has_down))
    def _():
        gx[own, pl.ds(rows, halo)] = jnp.zeros((halo, cols), bf16)

    @pl.when(jnp.logical_not(has_up))
    def _():
        gx[own, pl.ds(rows + halo, halo)] = jnp.zeros((halo, cols), bf16)

    for i in range(1, 5):
        w_copies[i].wait()
    wvt[...] = wv[...].astype(f32).T.astype(bf16)
    a_copy().wait_recv()

    def full_rows(at):
        return jnp.concatenate([gx[g, at] for g in range(groups)], axis=1).astype(f32)

    def norm(v, which):
        mean = jnp.mean(v, axis=-1, keepdims=True)
        spread = jnp.mean(v * v, axis=-1, keepdims=True) - mean * mean
        scaled = (v - mean) * lax.rsqrt(spread + NORM_EPS)
        return scaled * gains_ref[which : which + 1, :] + shifts_ref[which : which + 1, :]

    def project(i, keep):
        at = pl.ds(pl.multiple_of(i * chunk, chunk), chunk)
        normed = norm(full_rows(at), 0).astype(bf16)
        if keep:
            nbuf[at] = normed
        keys = jnp.dot(normed, wk[...], preferred_element_type=f32).astype(bf16)
        values = lax.dot_general(wvt[...], normed, NT, preferred_element_type=f32).astype(bf16)
        for k in range(per):
            kbuf[i * per + k] = keys[k * tile : (k + 1) * tile]
            vbuf[i * per + k] = values[:, k * tile : (k + 1) * tile]

    b_copy(0).wait_recv()
    c_copy(0).start()

    def own_step(i, carry):
        b_copy(i).wait_recv()
        c_copy(i).start()
        c_copy(i - 1).wait_recv()
        project(i - 1, True)
        return carry

    lax.fori_loop(1, n_own - 1, own_step, 0)

    @pl.when(has_down)
    def _():
        up_copy().wait_recv()

    @pl.when(has_up)
    def _():
        down_copy().wait_recv()

    b2_copy().start()
    a2_copy().start()
    lax.fori_loop(n_own - 1, n_own, own_step, 0)
    c_copy(n_own - 1).wait_recv()
    project(n_own - 1, True)

    scale = LOG2E / math.sqrt(HD)
    w_copies[5].wait()
    own_at = pl.ds(pl.multiple_of(s * half_rows, half_rows), half_rows)
    q_rows = jnp.dot(nbuf[own_at], wq[...], preferred_element_type=f32) * scale
    qbuf[...] = q_rows.astype(bf16)
    w_copies[6].wait()
    b2_copy().wait_recv()
    c2_copy().start()
    a2_copy().wait_recv()
    c2_copy().wait_recv()

    def halo_step(i, carry):
        project(i, False)
        return carry

    lax.fori_loop(n_own, n_own + n_halo, halo_step, 0)

    live = live_ref[0]
    word_rows = tile // words
    row_id = lax.broadcasted_iota(jnp.int32, (tile, tile), 0)
    col_id = lax.broadcasted_iota(jnp.int32, (tile, tile), 1)
    shifts = lax.broadcasted_iota(jnp.int32, (word_rows, tile), 0)
    low_half = lax.broadcasted_iota(jnp.int32, (tile, pw), 1) < HD

    def t_copy(j):
        at = pl.ds(j * tile, tile)
        return rdma(att.at[c, at], att.at[c, at], t_send.at[j], t_recv.at[j], xdev)

    ones = jnp.ones((16, 2 * tile), bf16)

    def attend_block(j, carry):
        b = s * blocks_here + j
        ids = [tk_ref[b, t] for t in range(slots)]
        q_rows = qbuf[pl.ds(pl.multiple_of(j * tile, tile), tile)]
        wide = []
        for pair in range(pairs):
            q_pair = q_rows[:, pair * pw : (pair + 1) * pw]
            zero = jnp.zeros_like(q_pair)
            wide.append(
                jnp.concatenate(
                    [jnp.where(low_half, q_pair, zero), jnp.where(low_half, zero, q_pair)], axis=0
                )
            )
        tops = [jnp.full((8, 2 * tile), NEG_FILL, f32) for _ in range(pairs)]
        for t in range(slots):
            block_bits = bits_ref[b, t]
            set_bits = jnp.concatenate(
                [
                    jnp.right_shift(
                        jnp.broadcast_to(block_bits[w : w + 1, :], (word_rows, tile)), shifts
                    )
                    & 1
                    for w in range(words)
                ],
                axis=0,
            )
            limit = jnp.where(ids[t] >= blocks_own, tile, live - ids[t] * tile)
            good = row_id < limit
            if t == 0:
                good = good | (row_id == col_id)
            bias = jnp.where((set_bits == 1) & good, 0.0, NEG_FILL)
            bias = jnp.concatenate([bias, bias], axis=1)
            for pair in range(pairs):
                keys = kbuf[ids[t], :, pair * pw : (pair + 1) * pw]
                scores = lax.dot_general(keys, wide[pair], NT, preferred_element_type=f32) + bias
                s_ref[pair, t * tile : (t + 1) * tile] = scores
                tops[pair] = jnp.maximum(
                    tops[pair], jnp.max(scores.reshape(tile // 8, 8, 2 * tile), axis=0)
                )
        pieces = []
        for pair in range(pairs):
            top = jnp.max(tops[pair], axis=0, keepdims=True)
            mixed = jnp.zeros((pw + 16, 2 * tile), f32)
            for t in range(0, slots, 2):
                p = jnp.exp2(s_ref[pair, t * tile : (t + 2) * tile] - top).astype(bf16)
                at = slice(pair * pw, (pair + 1) * pw)
                values = jnp.concatenate([vbuf[ids[t], at], vbuf[ids[t + 1], at]], axis=1)
                values = jnp.concatenate([values, ones], axis=0)
                mixed = mixed + jnp.dot(values, p, preferred_element_type=f32)
            inverse = 1.0 / mixed[pw : pw + 1]
            pieces.append(mixed[:HD, :tile] * inverse[:, :tile])
            pieces.append(mixed[HD:pw, tile:] * inverse[:, tile:])
        att[c, pl.ds(pl.multiple_of(j * tile, tile), tile)] = (
            jnp.concatenate(pieces, axis=0).T.astype(bf16)
        )
        t_copy(j).start()
        return carry

    lax.fori_loop(0, blocks_here, attend_block, 0)

    for i in (7, 8, 9):
        w_copies[i].wait()

    n_ffn = half_rows // chunk

    def p_copy(i):
        at = pl.ds(i * chunk, chunk)
        return rdma(psend.at[at], precv.at[at], p_send.at[i], p_recv.at[i], xdev)

    def ffn_chunk(i, carry):
        for k in range(per):
            t_copy(i * per + k).wait_recv()
        at = pl.ds(pl.multiple_of(i * chunk, chunk), chunk)
        rows_at = pl.ds(pl.multiple_of(s * half_rows + i * chunk, chunk), chunk)
        mixed = jnp.concatenate([att[g, at] for g in range(groups // 2)], axis=1)
        after = full_rows(rows_at) + jnp.dot(mixed, wo[...], preferred_element_type=f32)
        normed_two = norm(after, 1).astype(bf16)
        hidden = gelu_tanh(
            lax.dot_general(normed_two, fin[...], NT, preferred_element_type=f32)
        ).astype(bf16)
        part = jnp.dot(hidden, fout[...], preferred_element_type=f32)
        left, right = part[:, :head_cols], part[:, head_cols:]
        first = c == 0
        psend[at] = jnp.where(first, right, left).astype(bf16)
        p_copy(i).start()
        own_part[at] = jnp.where(first, left + after[:, :head_cols], right + after[:, head_cols:])
        return carry

    lax.fori_loop(0, n_ffn, ffn_chunk, 0)

    def o_copy(i):
        at = pl.ds(i * chunk, chunk)
        out_at = pl.ds(s * half_rows + i * chunk, chunk)
        return rdma(osend.at[at], out_ref.at[out_at], o_send.at[i], o_recv.at[i], sdev)

    def finish(i, carry):
        p_copy(i).wait_recv()
        at = pl.ds(pl.multiple_of(i * chunk, chunk), chunk)
        base = s * half_rows + i * chunk
        summed = own_part[at] + precv[at].astype(f32)
        position = base + lax.broadcasted_iota(jnp.int32, (chunk, head_cols), 0)
        done = jnp.where(position < live, summed, 0.0)
        left, right = done[:, :cols], done[:, cols:]
        first = s == 0
        osend[at] = jnp.where(first, right, left).astype(bf16)
        o_copy(i).start()
        out_ref[pl.ds(pl.multiple_of(base, chunk), chunk)] = jnp.where(
            first, left, right
        ).astype(bf16)
        return carry

    lax.fori_loop(0, n_ffn, finish, 0)

    a_copy().wait_send()
    a2_copy().wait_send()
    b2_copy().wait_send()
    c2_copy().wait_send()
    for i in range(n_own):
        b_copy(i).wait_send()
        c_copy(i).wait_send()
    for j in range(blocks_here):
        t_copy(j).wait_send()

    @pl.when(has_up)
    def _():
        up_copy().wait_send()

    @pl.when(has_down)
    def _():
        down_copy().wait_send()

    for i in range(n_ffn):
        p_copy(i).wait_send()
        o_copy(i).wait()


def one_kernel(*args):
    (x, gains, shifts, wq, wk, wv, wo, fin, fout, live, send, tk, bits) = args
    bf16 = jnp.bfloat16
    rows, cols = x.shape
    width = gains.shape[1]
    groups = lax.axis_size("chan") * lax.axis_size("sub")
    halo = send.shape[-1]
    tile = bits.shape[-1]
    slots = tk.shape[1]
    ext = rows + 2 * halo
    head_cols = wq.shape[1]
    half = rows // 2
    chunk = 2 * tile
    n_own = rows // chunk
    blocks_here = tk.shape[0] // 2
    n_ffn = half // chunk
    vmem = pltpu.VMEM
    dma = pltpu.SemaphoreType.DMA
    in_vmem = pl.BlockSpec(memory_space=pltpu.VMEM)
    in_smem = pl.BlockSpec(memory_space=pltpu.SMEM)
    in_any = pl.BlockSpec(memory_space=pl.ANY)
    return pl.pallas_call(
        layer_kernel,
        out_shape=pltpu.VMEM(x.shape, bf16),
        in_specs=[in_any] * 9 + [in_smem, in_any, in_smem, in_any],
        out_specs=in_vmem,
        scratch_shapes=[
            vmem((groups, ext, cols), bf16),
            vmem((2, halo, cols), bf16),
            vmem((rows, width), bf16),
            vmem((ext // tile, tile, head_cols), bf16),
            vmem((ext // tile, head_cols, tile), bf16),
            vmem((head_cols, width), bf16),
            vmem((half, head_cols), bf16),
            vmem((head_cols // (2 * HD), slots * tile, 2 * tile), jnp.float32),
            vmem((2, half, head_cols), bf16),
            vmem((half, head_cols), jnp.float32),
            vmem((half, head_cols), bf16),
            vmem((half, head_cols), bf16),
            vmem((half, cols), bf16),
            vmem(wq.shape, bf16),
            vmem(wk.shape, bf16),
            vmem(wv.shape, bf16),
            vmem(wo.shape, bf16),
            vmem(fin.shape, bf16),
            vmem(fout.shape, bf16),
            vmem(gains.shape, jnp.float32),
            vmem(shifts.shape, jnp.float32),
            vmem(send.shape, jnp.int32),
            vmem(bits.shape, jnp.int32),
            dma((10,)),
            dma,
            dma((2,)),
            dma((2,)),
            dma((n_own + 1,)),
            dma((n_own + 1,)),
            dma((n_own + 1,)),
            dma((n_own + 1,)),
            dma((2,)),
            dma((2,)),
            dma((blocks_here,)),
            dma((blocks_here,)),
            dma((n_ffn,)),
            dma((n_ffn,)),
            dma((n_ffn,)),
            dma((n_ffn,)),
        ],
        compiler_params=pltpu.CompilerParams(collective_id=0, has_side_effects=True),
    )(*args)


def on_any_device(*args):
    two_by_two = lax.axis_size("chan") == 2 and lax.axis_size("sub") == 2
    cols, head_cols = args[0].shape[1], args[3].shape[1]
    tile, halo = args[12].shape[-1], args[10].shape[-1]
    rows_fit = args[0].shape[0] % (4 * tile) == 0 and 2 * halo % (2 * tile) == 0
    if two_by_two and cols % 128 == 0 and head_cols % (2 * HD) == 0 and rows_fit and args[11].shape[1] % 2 == 0:
        return one_kernel(*args)
    return on_device(*args)


def solution(mesh):
    in_specs = (
        P(("ens", "space"), ("chan", "sub")),
        P(),
        P(),
        P(None, "chan"),
        P(None, "chan"),
        P(None, "chan"),
        P(),
        P("chan", None),
        P("chan", None),
        P("space"),
        P("space", None, None),
        P("space", None),
        P("space", None, None, None),
    )
    out_specs = P(("ens", "space"), ("chan", "sub"))
    return jax.shard_map(
        on_any_device, mesh=mesh, in_specs=in_specs, out_specs=out_specs, check_vma=False
    )
```
